256 devices in a mesh: seq: 16 (over z, core), head: 4 (over x), dp: 4 (over y).
Axes of the slice: x: 4, y: 4, z: 8, core: 2. Of those that a mesh axis runs over, the one named last changes fastest.
Arguments:
- queries: bfloat16 [4, 4096, 64, 128], P('dp', 'seq', 'head'), may hold values from -6 to 6
- keys: bfloat16 [4, 4096, 8, 128], P('dp', 'seq', 'head'), may hold values from -6 to 6
- values: bfloat16 [4, 4096, 8, 128], P('dp', 'seq', 'head'), may hold values from -6 to 6
- attn_out: bfloat16 [4, 4096, 64, 128], P('dp', 'seq', 'head'), may hold values from -6 to 6
- out_grad: bfloat16 [4, 4096, 64, 128], P('dp', 'seq', 'head'), may hold values from -6 to 6
- gate_values: float32 [4, 64, 4096], P('dp', 'head', 'seq'), may hold values from 0.05 to 0.95
- log_totals: float32 [4, 64, 4096], P('dp', 'head', 'seq'), may hold values from 3 to 5
- hidden: bfloat16 [4, 4096, 5120], P('dp', 'seq', 'head'), may hold values from -6 to 6
- block_ids: int32 [4, 64, 8, 16], P('dp', 'seq', 'head'), may hold values from 0 to 63, as said below
- block_valid: int32 [4, 64, 8, 16], P('dp', 'seq', 'head'), may hold values from 0 to 1
Outputs:
- query_grad: bfloat16 [4, 4096, 64, 128], P('dp', 'seq', 'head')
- key_grad: bfloat16 [4, 4096, 8, 128], P('dp', 'seq', 'head')
- value_grad: bfloat16 [4, 4096, 8, 128], P('dp', 'seq', 'head')
- gate_weight_grad: float32 [64, 5120], P(None, 'head')
The draws below stay inside these ranges and needn't reach their ends.
Inputs may be any that keep to these rules, and one draw needn't show every extreme that they name: `block_ids`: for query tile t and key head k, the slots whose block_valid is 1 name distinct blocks of index at most t, among them block t itself and block 0; exactly min(16, t + 1) slots are valid. The ids of the other slots are any blocks, and may repeat a valid one.
All inputs are finite; a program needn't handle non-finite values.
Results may differ from the reference program's by a relative error of at most 0.025.
Values may be sent and summed in bfloat16 or wider, within the bound.
A program may use at most 128 MiB of HBM per device.

```python
import jax
import jax.numpy as jnp
from jax import lax

D = 5120
HQ = 64
KVH = 8
DH = 128
BLK = 64
NSEL = 16
TOK_DEV = 256
GROUP = 8
BATCH = 4
SEQLEN = 4096
TILES = 64
N_SEQ = 16


def choose_blocks(key):
    seeded = jax.random.fold_in(key, 17)
    rank_key, order_key = jax.random.split(seeded)
    filler_key = jax.random.fold_in(seeded, 5)
    near_key, far_key, coin_key = jax.random.split(filler_key, 3)
    width_all = TILES + NSEL
    candidate = jnp.arange(width_all, dtype=jnp.int32)[None, None, None, :]
    tile_of = jnp.arange(TILES, dtype=jnp.int32)[None, :, None, None]
    random_part = jax.random.randint(rank_key, (BATCH, TILES, KVH, width_all), 0, 1 << 20)
    ranking = random_part * width_all + candidate
    ranking = jnp.where(candidate <= tile_of, ranking, -1 - candidate)
    ranking = jnp.where(candidate == 0, 1 << 30, ranking)
    ranking = jnp.where(candidate == tile_of, (1 << 30) + 1, ranking)
    best_scores, best_slots = lax.top_k(ranking, NSEL)
    usable = (best_scores >= 0).astype(jnp.int32)
    chosen = (best_slots % TILES).astype(jnp.int32)
    shuffle_keys = jax.random.randint(order_key, (BATCH, TILES, KVH, NSEL), 0, 1 << 20) * NSEL + jnp.arange(NSEL, dtype=jnp.int32)
    shuffle = jnp.argsort(shuffle_keys, axis=-1)
    chosen = jnp.take_along_axis(chosen, shuffle, axis=-1)
    usable = jnp.take_along_axis(usable, shuffle, axis=-1)
    slot_shape = (BATCH, TILES, KVH, NSEL)
    near = jax.random.randint(near_key, slot_shape, 0, 1 << 20) % (tile_of + 1)
    far = jax.random.randint(far_key, slot_shape, 0, TILES)
    coin = jax.random.randint(coin_key, slot_shape, 0, 2)
    filler = jnp.where(coin == 0, near, far).astype(jnp.int32)
    chosen = jnp.where(usable > 0, chosen, filler).astype(jnp.int32)
    return (chosen, usable)


def draw_block_ids(key, part):
    return choose_blocks(key)[0]


def draw_block_valid(key, part):
    return choose_blocks(key)[1]


def block_scale(key, dims, cuts, smallest, largest):
    loudness = 1.0
    for position, blocks in cuts:
        heights = jax.random.uniform(jax.random.fold_in(jax.random.fold_in(key, 6), position), (blocks,), jnp.float32, smallest / len(cuts), largest / len(cuts))
        loudness = loudness * jnp.repeat(jnp.exp(heights), dims[position] // blocks).reshape((-1,) + (1,) * (len(dims) - 1 - position))
    return loudness


def bell_draw(rng, extent, spread, limit, cuts=(), kind=jnp.bfloat16):
    drawn = jax.random.normal(rng, extent, jnp.float32) * spread
    if len(cuts) > 0:
        drawn = block_scale(rng, extent, cuts, -0.22, 0.18) * drawn
    return jnp.clip(drawn, min=-limit, max=limit).astype(kind)


def setup_inputs(seed: int = 0) -> dict:
    splits = jax.random.split(jax.random.key(seed), 11)
    return {
        "queries": bell_draw(splits[0], (BATCH, SEQLEN, HQ, DH), 1.0, 6.0, ((0, 4), (1, 16), (2, 4))),
        "keys": bell_draw(splits[1], (BATCH, SEQLEN, KVH, DH), 1.0, 6.0, ((0, 4), (1, 16), (2, 4))),
        "values": bell_draw(splits[2], (BATCH, SEQLEN, KVH, DH), 1.0, 6.0, ((0, 4), (1, 16), (2, 4))),
        "attn_out": bell_draw(splits[3], (BATCH, SEQLEN, HQ, DH), 1.0, 6.0, ((0, 4), (1, 16), (2, 4))),
        "out_grad": bell_draw(splits[4], (BATCH, SEQLEN, HQ, DH), 1.0, 6.0, ((0, 4), (1, 16), (2, 4))),
        "gate_values": jnp.clip(0.05 + 0.9 * jax.random.uniform(splits[5], (BATCH, HQ, SEQLEN), jnp.float32) ** block_scale(splits[5], (BATCH, HQ, SEQLEN), ((0, 4), (1, 4), (2, 16)), -0.2, 0.2), 0.05, 0.95),
        "log_totals": jnp.clip(3.0 + 2.0 * jax.random.uniform(splits[6], (BATCH, HQ, SEQLEN), jnp.float32) ** block_scale(splits[6], (BATCH, HQ, SEQLEN), ((0, 4), (1, 4), (2, 16)), -0.2, 0.2), 3.0, 5.0),
        "hidden": bell_draw(splits[7], (BATCH, SEQLEN, D), 1.0, 6.0, ((0, 4), (1, 16), (2, 4))),
        "block_ids": draw_block_ids(jax.random.fold_in(splits[10], 71), 0),
        "block_valid": draw_block_valid(jax.random.fold_in(splits[10], 71), 0),
    }


def reference(queries, keys, values, attn_out, out_grad, gate_values, log_totals, hidden, block_ids, block_valid):
    factor = DH ** -0.5
    tiles_dev = TOK_DEV // BLK
    key_blocks = keys.reshape(BATCH, TILES, BLK, KVH, DH)
    value_blocks = values.reshape(BATCH, TILES, BLK, KVH, DH)
    batch_index = jnp.arange(BATCH, dtype=jnp.int32)[:, None, None]
    kv_index = jnp.arange(KVH, dtype=jnp.int32)[None, :, None]
    offsets = jnp.arange(BLK, dtype=jnp.int32)

    def tile_step(partial_value, tile_index):
        first_row = tile_index * BLK
        query_tile = lax.dynamic_slice_in_dim(queries, first_row, BLK, 1).reshape(BATCH, BLK, KVH, GROUP, DH).astype(jnp.float32)
        output_tile = lax.dynamic_slice_in_dim(attn_out, first_row, BLK, 1).reshape(BATCH, BLK, KVH, GROUP, DH).astype(jnp.float32)
        upstream = lax.dynamic_slice_in_dim(out_grad, first_row, BLK, 1).reshape(BATCH, BLK, KVH, GROUP, DH).astype(jnp.float32)
        gate_tile = lax.dynamic_slice_in_dim(gate_values, first_row, BLK, 2).reshape(BATCH, KVH, GROUP, BLK)
        totals = lax.dynamic_slice_in_dim(log_totals, first_row, BLK, 2).reshape(BATCH, KVH, GROUP, BLK)
        chosen = lax.dynamic_index_in_dim(block_ids, tile_index, 1, keepdims=False)
        usable = lax.dynamic_index_in_dim(block_valid, tile_index, 1, keepdims=False) > 0
        key_sel = key_blocks[batch_index, chosen, :, kv_index, :].astype(jnp.float32)
        value_sel = value_blocks[batch_index, chosen, :, kv_index, :].astype(jnp.float32)
        gates_by_row = jnp.transpose(gate_tile, (0, 3, 1, 2))
        grad_low = lax.optimization_barrier((gates_by_row[..., None] * upstream).astype(jnp.bfloat16))
        grad_output = grad_low.astype(jnp.float32)
        row_delta = jnp.transpose(jnp.sum(grad_output * output_tile, axis=-1), (0, 2, 3, 1))
        gate_grad = jnp.sum(upstream * output_tile, axis=-1)
        logit_grad = (gate_grad * gates_by_row * (1.0 - gates_by_row)).astype(jnp.bfloat16)
        scores = jnp.einsum("bikgd,bknjd->bkginj", query_tile, key_sel) * factor
        query_pos = first_row + offsets
        key_pos = chosen[..., None] * BLK + offsets
        allowed = usable[:, :, None, :, None] & (key_pos[:, :, None, :, :] <= query_pos[None, None, :, None, None])
        probability = jnp.where(allowed[:, :, None], jnp.exp(scores - totals[..., None, None]), 0.0)
        prob_grad = jnp.einsum("bikgd,bknjd->bkginj", grad_output, value_sel)
        dscore = lax.optimization_barrier((probability * (prob_grad - row_delta[..., None, None])).astype(jnp.bfloat16)).astype(jnp.float32)
        prob_low = lax.optimization_barrier(probability.astype(jnp.bfloat16)).astype(jnp.float32)
        query_part = (jnp.einsum("bkginj,bknjd->bikgd", dscore, key_sel) * factor).astype(jnp.bfloat16)
        key_part = jnp.einsum("bkginj,bikgd->bknjd", dscore, query_tile) * factor
        value_part = jnp.einsum("bkginj,bikgd->bknjd", prob_low, grad_output)
        partial_value = partial_value.at[batch_index, chosen, :, kv_index, :].add(jnp.concatenate([key_part, value_part], axis=-1))
        return partial_value, (query_part, logit_grad)

    def source_step(total, source):
        tile_ids = source * tiles_dev + jnp.arange(tiles_dev, dtype=jnp.int32)
        fresh = jnp.zeros((BATCH, TILES, BLK, KVH, 2 * DH), jnp.float32)
        partial_value, parts = lax.scan(tile_step, fresh, tile_ids)
        rounded = lax.optimization_barrier(partial_value.astype(jnp.bfloat16)).astype(jnp.float32)
        return total + rounded, parts

    start_total = jnp.zeros((BATCH, TILES, BLK, KVH, 2 * DH), jnp.float32)
    summed_all, (query_parts, logit_parts) = lax.scan(source_step, start_total, jnp.arange(N_SEQ, dtype=jnp.int32))
    query_parts = query_parts.reshape((TILES,) + query_parts.shape[2:])
    logit_parts = logit_parts.reshape((TILES,) + logit_parts.shape[2:])
    query_grad = jnp.swapaxes(query_parts, 0, 1).reshape(BATCH, SEQLEN, HQ, DH)
    logit_rows = jnp.transpose(logit_parts.reshape(TILES, BATCH, BLK, HQ), (3, 1, 0, 2)).reshape(HQ, BATCH * SEQLEN)
    gate_weight_grad = jnp.dot(logit_rows, hidden.reshape(BATCH * SEQLEN, D), preferred_element_type=jnp.float32) * (1.0 / (BATCH * SEQLEN) ** 0.5)
    summed = summed_all.reshape(BATCH, SEQLEN, KVH, 2 * DH)
    return query_grad, summed[..., :DH].astype(jnp.bfloat16), summed[..., DH:].astype(jnp.bfloat16), gate_weight_grad
```

```python
import jax
import jax.numpy as jnp
from jax import lax
from jax.experimental import pallas as pl
from jax.experimental.pallas import tpu as pltpu
from jax.sharding import PartitionSpec as P

F32, BF16 = jnp.float32, jnp.bfloat16
MESH = pl.DeviceIdType.MESH
LOG2E = 1.4426950408889634
FACTOR = 128**-0.5
NZ, NX, NY = 8, 4, 4
TILES, SLOTS, GROUP = 4, 16, 4
SCALE = 1.0 / (4 * 4096) ** 0.5


def nt(a, b):
    return lax.dot_general(a, b, (((1,), (1,)), ((), ())), preferred_element_type=F32)


def nn(a, b):
    return jnp.dot(a, b, preferred_element_type=F32)


def tn(a, b):
    return lax.dot_general(a, b, (((0,), (0,)), ((), ())), preferred_element_type=F32)


def split3(x):
    hi = x.astype(BF16)
    rest = x - hi.astype(F32)
    mid = rest.astype(BF16)
    return hi, mid, (rest - mid.astype(F32)).astype(BF16)


def prepass(q_ref, u_ref, o_ref, gate_ref, tot_ref, qs, us, arow, drow, logit_ref):
    gate = gate_ref[...]
    shift = jnp.concatenate(split3((tot_ref[...] - jnp.log(gate)) * LOG2E), axis=0)
    token = lax.broadcasted_iota(jnp.int32, (256, 512), 0)
    lane = lax.broadcasted_iota(jnp.int32, (256, 512), 1)
    own = lax.broadcasted_iota(jnp.int32, (8, 512), 0) == lax.broadcasted_iota(jnp.int32, (8, 512), 1) % 8
    ones = jnp.ones((8, 256), BF16)
    for t in range(TILES):
        pick = jnp.where(token == 64 * t + lane // 8, 1.0, 0.0).astype(BF16)
        spread = nn(shift, pick)
        spread = spread[0:16] + spread[16:32] + spread[32:48]
        rows = pl.ds(64 * t, 64)
        up = u_ref[rows].astype(F32)
        prod = up * o_ref[rows].astype(F32)
        query = q_ref[rows].astype(F32)
        for h in range(2):
            heads = slice(8 * h, 8 * h + 8)
            qs[h, t] = query[:, heads, :].reshape(512, 128).astype(BF16)
            us[h, t] = up[:, heads, :].reshape(512, 128).astype(BF16)
            p = prod[:, heads, :].reshape(512, 128)
            high = p.astype(BF16)
            low = (p - high.astype(F32)).astype(BF16)
            delta = nt(ones, jnp.concatenate([high, low], axis=1))
            drow[h, t] = delta
            arow[h, t] = jnp.broadcast_to(jnp.sum(jnp.where(own, spread[heads], 0.0), axis=0, keepdims=True), (8, 512))
            mine = jnp.where(own, delta, 0.0)
            high = mine.astype(BF16)
            low = (mine - high.astype(F32)).astype(BF16)
            back = nt(jnp.concatenate([high, low], axis=0), pick)
            back = back[0:8] + back[8:16]
            if t == 0:
                logit_ref[heads, :] = back
            else:
                logit_ref[heads, :] += back
    return logit_ref[...] * gate * (1.0 - gate)


def attend(h, t, tile_number, ids, valid, kbuf, qs, us, arow, drow, dqs, ck, cv):
    query, up = qs[h, t], us[h, t]
    shift, delta = arow[h, t][0:1], drow[h, t][0:1]
    ahead = lax.broadcasted_iota(jnp.int32, (64, 512), 1) // 8 - lax.broadcasted_iota(jnp.int32, (64, 512), 0)
    dq = None
    for first in range(0, SLOTS, GROUP):
        picked = [ids[t, h, first + k] for k in range(GROUP)]
        key = jnp.concatenate([kbuf[0, m] for m in picked], axis=0)
        value = jnp.concatenate([kbuf[1, m] for m in picked], axis=0)
        score = nt(key, query)
        grad = nt(value, up)
        probs, dscores = [], []
        for k in range(GROUP):
            least = jnp.where(valid[t, h, first + k] > 0, (picked[k] - tile_number) * 64, 1 << 20)
            part = slice(64 * k, 64 * k + 64)
            prob = jnp.exp2(jnp.where(ahead >= least, score[part] * (FACTOR * LOG2E) - shift, -jnp.inf))
            probs.append(prob.astype(BF16))
            dscores.append((prob * (grad[part] - delta)).astype(BF16))
        prob = jnp.concatenate(probs, axis=0)
        dscore = jnp.concatenate(dscores, axis=0)
        dv = nn(prob, up)
        dk = nn(dscore, query)
        for k in range(GROUP):
            cv[t, first + k] = dv[64 * k : 64 * k + 64]
            ck[t, first + k] = dk[64 * k : 64 * k + 64]
        more = tn(key, dscore)
        dq = more if dq is None else dq + more
    dqs[h, t] = (dq * FACTOR).T


def kernel(
    ids, valid, inv, kv_hbm, q_hbm, u_hbm, o_hbm, gate_ref, tot_ref, hid_hbm,
    dq_hbm, dkv_hbm, gw_hbm,
    k0, k1, q_ref, u_ref, o_ref, hid, qs, us, arow, drow, dqs, logit_ref,
    ck0, cv0, ck1, cv1, pp_out, pp_in, rs_out, rs_in, dkv, dq_out,
    lall, gs, pb, hb, yb, z3, zin, full, gw,
    load_sem, store_sem, own_sem, ag_send, ag_recv, dd_send, dd_recv, pp_send, pp_recv, rs_send, rs_recv,
    lx_send, lx_recv, gp_send, gp_recv, ys_send, ys_recv, zs_send, zs_recv, zg_send, zg_recv, yg_send, yg_recv,
):
    s = lax.axis_index("seq")
    x = lax.axis_index("head")
    y = lax.axis_index("dp")
    z = s // 2
    c = s % 2
    partner = {"seq": 2 * z + (1 - c)}
    kbufs, cks, cvs = (k0, k1), (ck0, ck1), (cv0, cv1)

    def chip(j):
        return lax.rem(z + j + NZ, NZ)

    def zdev(j):
        return {"seq": 2 * chip(j) + c}

    def xdev(d):
        return {"head": lax.rem(x + d, NX)}

    def ydev(d):
        return {"dp": lax.rem(y + d, NY)}

    pending = []

    def send(src, dst, send_sem, recv_sem, device):
        copy = pltpu.make_async_remote_copy(
            src_ref=src, dst_ref=dst, send_sem=send_sem, recv_sem=recv_sem, device_id=device, device_id_type=MESH
        )
        copy.start()
        pending.append(copy)

    def arrived(dst, send_sem, recv_sem, device):
        pltpu.make_async_remote_copy(
            src_ref=dst, dst_ref=dst, send_sem=send_sem, recv_sem=recv_sem, device_id=device, device_id_type=MESH
        ).wait_recv()

    own = [
        pltpu.make_async_copy(kv_hbm.at[h, i], kbufs[h].at[i, pl.ds(4 * s, 4)], own_sem.at[h, i])
        for h in range(2) for i in range(2)
    ]
    loads = [
        pltpu.make_async_copy(a, b, load_sem.at[i])
        for i, (a, b) in enumerate(((q_hbm, q_ref), (u_hbm, u_ref), (o_hbm, o_ref), (hid_hbm, hid)))
    ]
    for copy in own + loads:
        copy.start()

    barrier = pltpu.get_barrier_semaphore()
    peers = [partner] + [zdev(j) for j in range(1, NZ)] + [xdev(d) for d in range(1, NX)] + [ydev(d) for d in range(1, NY)]
    for peer in peers:
        pl.semaphore_signal(barrier, inc=1, device_id=peer, device_id_type=MESH)
    pl.semaphore_wait(barrier, len(peers))

    def span(j, core):
        return pl.ds(4 * (2 * chip(j) + core), 4)

    def along(h, k, up, i):
        j = -k if up else k
        at = kbufs[h].at[i, span(j, c)]
        rel = (NZ - (k + 1)) if up else (k + 1)
        lane = 0 if up else 1
        send(at, at, ag_send.at[h, lane, k, i], ag_recv.at[h, rel, i], zdev(1 if up else -1))

    def share(h, j, i):
        at = kbufs[h].at[i, span(j, c)]
        send(at, at, dd_send.at[h, j % NZ, i], dd_recv.at[h, j % NZ, i], partner)

    def take(h, rel, i):
        j = rel
        at = kbufs[h].at[i, span(j, c)]
        arrived(at, ag_send.at[h, 0, 0, i], ag_recv.at[h, rel, i], partner)

    def gather_start(h):
        for i in range(2):
            along(h, 0, True, i)
            along(h, 0, False, i)
        for i in range(2):
            share(h, 0, i)

    def gather_hop(h, k):
        for i in (0, 1):
            if k < 4 or i == 0:
                take(h, NZ - k, i)
                if k < 3 or (k == 3 and i == 0):
                    along(h, k, True, i)
            if k < 4 or i == 1:
                take(h, k, i)
                if k < 3 or (k == 3 and i == 1):
                    along(h, k, False, i)
        for i in (0, 1):
            if k < 4 or i == 0:
                share(h, -k, i)
            if k < 4 or i == 1:
                if k < 4:
                    share(h, k, i)
                else:
                    share(h, -k, i)

    def gather_end(h):
        for j in range(NZ):
            for i in range(2):
                at = kbufs[h].at[i, span(j, 1 - c)]
                arrived(at, dd_send.at[h, j, i], dd_recv.at[h, j, i], partner)

    def term(h, i, owner, b):
        source = (cks, cvs)[i][h]
        total = None
        for t in range(TILES):
            one = source[t, inv[t, h, 4 * owner + b]]
            total = one if total is None else total + one
        return total * FACTOR if i == 0 else total

    def halves(h):
        for j in (4, 3, -3, 2, -2, 1, -1, 0):
            owner = 2 * chip(j) + (1 - c)
            for i in range(2):
                for b in range(4):
                    pp_out[h, j % NZ, i, b] = term(h, i, owner, b).astype(BF16)
                send(pp_out.at[h, j % NZ, i], pp_in.at[h, j % NZ, i], pp_send.at[h, j % NZ, i], pp_recv.at[h, j % NZ, i], partner)

    def scatter_step(h, k, up, i, received):
        j = k if up else -k
        lane = 0 if up else 1
        owner = 2 * chip(j) + c
        arrived(pp_in.at[h, j % NZ, i], pp_send.at[h, j % NZ, i], pp_recv.at[h, j % NZ, i], partner)
        if received:
            arrived(rs_in.at[h, lane, k, i], rs_send.at[h, lane, k, i], rs_recv.at[h, lane, k, i], partner)
        for b in range(4):
            total = term(h, i, owner, b) + pp_in[h, j % NZ, i, b].astype(F32)
            if received:
                total = total + rs_in[h, lane, k, i, b].astype(F32)
            rs_out[h, lane, k - 1, i, b] = total.astype(BF16)
        send(
            rs_out.at[h, lane, k - 1, i], rs_in.at[h, lane, k - 1, i],
            rs_send.at[h, lane, k - 1, i], rs_recv.at[h, lane, k - 1, i], zdev(1 if up else -1),
        )

    def scatter_start(h):
        scatter_step(h, 4, True, 0, False)
        scatter_step(h, 4, False, 1, False)
        scatter_step(h, 3, True, 1, False)
        scatter_step(h, 3, False, 0, False)

    def scatter_hop(h, k):
        if k == 3:
            scatter_step(h, 3, True, 0, True)
            scatter_step(h, 3, False, 1, True)
        else:
            scatter_step(h, k, True, 1, True)
            scatter_step(h, k, False, 0, True)
            scatter_step(h, k, True, 0, True)
            scatter_step(h, k, False, 1, True)

    def scatter_end(h):
        for i in range(2):
            arrived(pp_in.at[h, 0, i], pp_send.at[h, 0, i], pp_recv.at[h, 0, i], partner)
            for lane in range(2):
                arrived(rs_in.at[h, lane, 0, i], rs_send.at[h, lane, 0, i], rs_recv.at[h, lane, 0, i], partner)
            for b in range(4):
                total = term(h, i, s, b) + pp_in[h, 0, i, b].astype(F32)
                total = total + rs_in[h, 0, 0, i, b].astype(F32) + rs_in[h, 1, 0, i, b].astype(F32)
                dkv[i, h, b] = total.astype(BF16)

    def gate_logits(logit):
        lall[x] = logit.astype(BF16)
        for d in range(1, NX):
            send(lall.at[x], lall.at[x], lx_send.at[d - 1], lx_recv.at[d - 1], xdev(d))

    def gate_product():
        for d in range(1, NX):
            arrived(lall.at[lax.rem(x + NX - d, NX)], lx_send.at[d - 1], lx_recv.at[d - 1], partner)
        for r in range(2):
            gs[r] = nn(lall[2 * r : 2 * r + 2].reshape(32, 256), hid[...])
        send(gs.at[1 - c], pb, gp_send.at[0], gp_recv.at[0], partner)

    def gate_y():
        arrived(pb, gp_send.at[0], gp_recv.at[0], partner)
        both = gs[c] + pb[...]
        for r in range(NY):
            hb[r] = both[8 * r : 8 * r + 8]
        for d in range(1, NY):
            send(hb.at[lax.rem(y + d, NY)], yb.at[d - 1], ys_send.at[d - 1], ys_recv.at[d - 1], ydev(d))

    def gate_z():
        for d in range(1, NY):
            arrived(yb.at[d - 1], ys_send.at[d - 1], ys_recv.at[d - 1], partner)
        rows = hb[y] + yb[0] + yb[1] + yb[2]
        for r in range(NZ):
            z3[r] = rows[r : r + 1]
        for d in range(1, NZ):
            send(z3.at[chip(d)], zin.at[d - 1], zs_send.at[d - 1], zs_recv.at[d - 1], zdev(d))

    def gate_row():
        row = z3[z]
        for d in range(1, NZ):
            arrived(zin.at[d - 1], zs_send.at[d - 1], zs_recv.at[d - 1], partner)
            row = row + zin[d - 1]
        full[c, y, z] = row * SCALE
        for d in range(1, NZ):
            send(full.at[c, y, z], full.at[c, y, z], zg_send.at[d - 1], zg_recv.at[d - 1], zdev(d))

    def gate_back_y():
        for d in range(1, NZ):
            arrived(full.at[c, y, chip(-d)], zg_send.at[d - 1], zg_recv.at[d - 1], partner)
        for d in range(1, NY):
            send(full.at[c, y], full.at[c, y], yg_send.at[d - 1], yg_recv.at[d - 1], ydev(d))

    def gate_back():
        for d in range(1, NY):
            arrived(full.at[c, lax.rem(y + NY - d, NY)], yg_send.at[d - 1], yg_recv.at[d - 1], partner)
        send(full.at[c], full.at[c], gp_send.at[1], gp_recv.at[1], partner)

    def gate_end():
        arrived(full.at[1 - c], gp_send.at[1], gp_recv.at[1], partner)
        for r in range(64):
            gw[r : r + 1, :] = full[r // 32, r // 8 % 4, r % 8]

    def tile(h, t):
        attend(h, t, 4 * s + t, ids, valid, kbufs[h], qs, us, arow, drow, dqs, cks[h], cvs[h])

    for copy in own[:2]:
        copy.wait()
    gather_start(0)
    for h in range(2):
        for t in range(TILES):
            cks[h][t, SLOTS] = jnp.zeros((64, 128), F32)
            cvs[h][t, SLOTS] = jnp.zeros((64, 128), F32)
    for copy in loads:
        copy.wait()
    gate_logits(prepass(q_ref, u_ref, o_ref, gate_ref, tot_ref, qs, us, arow, drow, logit_ref))
    gather_hop(0, 1)
    gate_product()
    gather_hop(0, 2)
    gate_y()
    gather_hop(0, 3)
    for copy in own[2:]:
        copy.wait()
    gather_start(1)
    gate_z()
    gather_hop(0, 4)
    gather_end(0)
    tile(0, 0)
    gather_hop(1, 1)
    gate_row()
    tile(0, 1)
    gather_hop(1, 2)
    gate_back_y()
    tile(0, 2)
    gather_hop(1, 3)
    gate_back()
    tile(0, 3)
    halves(0)
    gather_hop(1, 4)
    scatter_start(0)
    gather_end(1)
    tile(1, 0)
    scatter_hop(0, 3)
    tile(1, 1)
    scatter_hop(0, 2)
    tile(1, 2)
    scatter_hop(0, 1)
    tile(1, 3)
    halves(1)
    scatter_start(1)
    for t in range(TILES):
        pair = jnp.concatenate([dqs[h, t].reshape(64, 8, 128) for h in range(2)], axis=1)
        dq_out[pl.ds(64 * t, 64)] = pair.astype(BF16)
    stores = [pltpu.make_async_copy(dq_out, dq_hbm, store_sem.at[0])]
    stores[0].start()
    scatter_hop(1, 3)
    gate_end()
    stores.append(pltpu.make_async_copy(gw, gw_hbm, store_sem.at[1]))
    stores[1].start()
    scatter_end(0)
    scatter_hop(1, 2)
    scatter_hop(1, 1)
    scatter_end(1)
    stores.append(pltpu.make_async_copy(dkv, dkv_hbm, store_sem.at[2]))
    stores[2].start()
    for copy in stores:
        copy.wait()
    for copy in pending:
        copy.wait_send()


def on_device(queries, keys, values, attn_out, out_grad, gate_values, log_totals, hidden, block_ids, block_valid):
    ids, valid = block_ids[0], block_valid[0]
    blocks = jnp.arange(64, dtype=jnp.int32)
    slots = jnp.arange(SLOTS, dtype=jnp.int32)
    hit = (ids[..., None] == blocks) & (valid[..., None] > 0)
    inv = SLOTS + jnp.sum(jnp.where(hit, slots[:, None] - SLOTS, 0), axis=2)
    kv = jnp.transpose(jnp.concatenate([keys, values], axis=0), (2, 0, 1, 3)).reshape(2, 2, 4, 64, 128)
    smem, vmem, hbm = (pl.BlockSpec(memory_space=m) for m in (pltpu.SMEM, pltpu.VMEM, pl.ANY))
    dma = pltpu.SemaphoreType.DMA
    piece = (4, 64, 128)
    dq, dkv, gw = pl.pallas_call(
        kernel,
        in_specs=[smem] * 3 + [hbm] * 4 + [vmem] * 2 + [hbm],
        out_specs=[hbm] * 3,
        out_shape=[
            jax.ShapeDtypeStruct((256, 16, 128), BF16),
            jax.ShapeDtypeStruct((2, 2, *piece), BF16),
            jax.ShapeDtypeStruct((64, 1280), F32),
        ],
        scratch_shapes=[pltpu.VMEM((2, 64, 64, 128), BF16)] * 2
        + [pltpu.VMEM((256, 16, 128), BF16)] * 3
        + [pltpu.VMEM((256, 1280), BF16)]
        + [pltpu.VMEM((2, TILES, 512, 128), BF16)] * 2
        + [pltpu.VMEM((2, TILES, 8, 512), F32)] * 2
        + [pltpu.VMEM((2, TILES, 512, 128), F32), pltpu.VMEM((16, 256), F32)]
        + [pltpu.VMEM((TILES, SLOTS + 1, 64, 128), F32)] * 4
        + [pltpu.VMEM((2, NZ, 2, *piece), BF16)] * 2
        + [pltpu.VMEM((2, 2, 4, 2, *piece), BF16)] * 2
        + [pltpu.VMEM((2, 2, *piece), BF16), pltpu.VMEM((256, 16, 128), BF16)]
        + [
            pltpu.VMEM((4, 16, 256), BF16),
            pltpu.VMEM((2, 32, 1280), F32),
            pltpu.VMEM((32, 1280), F32),
            pltpu.VMEM((4, 8, 1280), F32),
            pltpu.VMEM((3, 8, 1280), F32),
            pltpu.VMEM((8, 1, 1280), F32),
            pltpu.VMEM((7, 1, 1280), F32),
            pltpu.VMEM((2, 4, 8, 1, 1280), F32),
            pltpu.VMEM((64, 1280), F32),
        ]
        + [dma((4,)), dma((3,)), dma((2, 2))]
        + [dma((2, 2, 4, 2)), dma((2, NZ, 2))]
        + [dma((2, NZ, 2))] * 4
        + [dma((2, 2, 4, 2))] * 2
        + [dma((3,))] * 2
        + [dma((2,))] * 2
        + [dma((3,))] * 2
        + [dma((7,))] * 4
        + [dma((3,))] * 2,
        compiler_params=pltpu.CompilerParams(collective_id=0, has_side_effects=True, vmem_limit_bytes=62 << 20),
        name="sparse_backward",
    )(ids, valid, inv, kv, queries[0], out_grad[0], attn_out[0], gate_values[0], log_totals[0], hidden[0])
    pair = jnp.transpose(dkv.reshape(2, 2, 256, 128), (0, 2, 1, 3))
    return dq[None], pair[0][None], pair[1][None], gw


def solution(mesh):
    wide = P("dp", "seq", "head", None)
    rows = P("dp", "head", "seq")
    return jax.shard_map(
        on_device,
        mesh=mesh,
        in_specs=(wide, wide, wide, wide, wide, rows, rows, P("dp", "seq", "head"), wide, wide),
        out_specs=(wide, wide, wide, P(None, "head")),
        check_vma=False,
    )
```

```python
import jax
import jax.numpy as jnp
from jax import lax
from jax.experimental import pallas as pl
from jax.experimental.pallas import tpu as pltpu
from jax.sharding import PartitionSpec as P

F32, BF16 = jnp.float32, jnp.bfloat16
MESH = pl.DeviceIdType.MESH
LOG2E = 1.4426950408889634
FACTOR = 128**-0.5
NZ, NX, NY = 8, 4, 4
TILES, SLOTS, GROUP = 4, 16, 4
UP, DOWN = (0, 1, 2, 3), (2, 3, 0, 1)
SCALE = 1.0 / (4 * 4096) ** 0.5


def nt(a, b):
    return lax.dot_general(a, b, (((1,), (1,)), ((), ())), preferred_element_type=F32)


def nn(a, b):
    return jnp.dot(a, b, preferred_element_type=F32)


def tn(a, b):
    return lax.dot_general(a, b, (((0,), (0,)), ((), ())), preferred_element_type=F32)


def split3(x):
    hi = x.astype(BF16)
    rest = x - hi.astype(F32)
    mid = rest.astype(BF16)
    return hi, mid, (rest - mid.astype(F32)).astype(BF16)


def prepass(q_ref, u_ref, o_ref, gate_ref, tot_ref, qs, us, arow, drow, logit_ref):
    gate = gate_ref[...]
    shift = jnp.concatenate(split3((tot_ref[...] - jnp.log(gate)) * LOG2E), axis=0)
    token = lax.broadcasted_iota(jnp.int32, (256, 512), 0)
    lane = lax.broadcasted_iota(jnp.int32, (256, 512), 1)
    own = lax.broadcasted_iota(jnp.int32, (8, 512), 0) == lax.broadcasted_iota(jnp.int32, (8, 512), 1) % 8
    ones = jnp.ones((8, 256), BF16)
    for t in range(TILES):
        pick = jnp.where(token == 64 * t + lane // 8, 1.0, 0.0).astype(BF16)
        spread = nn(shift, pick)
        spread = spread[0:16] + spread[16:32] + spread[32:48]
        rows = pl.ds(64 * t, 64)
        up = u_ref[rows].astype(F32)
        prod = up * o_ref[rows].astype(F32)
        query = q_ref[rows].astype(F32)
        for h in range(2):
            heads = slice(8 * h, 8 * h + 8)
            qs[h, t] = query[:, heads, :].reshape(512, 128).astype(BF16)
            us[h, t] = up[:, heads, :].reshape(512, 128).astype(BF16)
            p = prod[:, heads, :].reshape(512, 128)
            high = p.astype(BF16)
            low = (p - high.astype(F32)).astype(BF16)
            delta = nt(ones, jnp.concatenate([high, low], axis=1))
            drow[h, t] = delta
            arow[h, t] = jnp.broadcast_to(jnp.sum(jnp.where(own, spread[heads], 0.0), axis=0, keepdims=True), (8, 512))
            mine = jnp.where(own, delta, 0.0)
            high = mine.astype(BF16)
            low = (mine - high.astype(F32)).astype(BF16)
            back = nt(jnp.concatenate([high, low], axis=0), pick)
            back = back[0:8] + back[8:16]
            if t == 0:
                logit_ref[heads, :] = back
            else:
                logit_ref[heads, :] += back
    return logit_ref[...] * gate * (1.0 - gate)


def attend(h, t, tile_number, ids, valid, kbuf, qs, us, arow, drow, dqs, ck, cv, between):
    query, up = qs[h, t], us[h, t]
    shift, delta = arow[h, t][0:1], drow[h, t][0:1]
    ahead = lax.broadcasted_iota(jnp.int32, (64, 512), 1) // 8 - lax.broadcasted_iota(jnp.int32, (64, 512), 0)
    dq = None
    for first in range(0, SLOTS, GROUP):
        picked = [ids[t, h, first + k] for k in range(GROUP)]
        key = jnp.concatenate([kbuf[0, m] for m in picked], axis=0)
        value = jnp.concatenate([kbuf[1, m] for m in picked], axis=0)
        score = nt(key, query)
        grad = nt(value, up)
        probs, dscores = [], []
        for k in range(GROUP):
            least = jnp.where(valid[t, h, first + k] > 0, (picked[k] - tile_number) * 64, 1 << 20)
            part = slice(64 * k, 64 * k + 64)
            prob = jnp.exp2(jnp.where(ahead >= least, score[part] * (FACTOR * LOG2E) - shift, -jnp.inf))
            probs.append(prob.astype(BF16))
            dscores.append((prob * (grad[part] - delta)).astype(BF16))
        prob = jnp.concatenate(probs, axis=0)
        dscore = jnp.concatenate(dscores, axis=0)
        dv = nn(prob, up)
        dk = nn(dscore, query)
        for k in range(GROUP):
            cv[t, first + k] = dv[64 * k : 64 * k + 64]
            ck[t, first + k] = dk[64 * k : 64 * k + 64]
        more = tn(key, dscore)
        dq = more if dq is None else dq + more
        if first // GROUP % 2 == 1:
            between()
    dqs[h, t] = (dq * FACTOR).T


def kernel(
    ids, valid, k_hbm, v_hbm, q_hbm, u_hbm, o_hbm, gate_ref, tot_ref, hid_hbm,
    dq_hbm, dk_hbm, dv_hbm, gw_hbm,
    k_in, v_in, inv_v, inv, k0, k1, q_ref, u_ref, o_ref, hid, qs, us, arow, drow, dqs, logit_ref,
    ck0, cv0, ck1, cv1, pp_out, pp_in, rs_out, rs_in, dkv, dk_out, dv_out, dq_out,
    lall, gs, pb, hb, yb, z3, zin, full, gw,
    load_sem, store_sem, own_sem, inv_sem, ag_send, ag_recv, dd_send, dd_recv, pp_send, pp_recv, rs_send, rs_recv,
    lx_send, lx_recv, gp_send, gp_recv, ys_send, ys_recv, zs_send, zs_recv, zg_send, zg_recv, yg_send, yg_recv,
):
    s = lax.axis_index("seq")
    x = lax.axis_index("head")
    y = lax.axis_index("dp")
    z = s // 2
    c = s % 2
    partner = {"seq": 2 * z + (1 - c)}
    kbufs, cks, cvs = (k0, k1), (ck0, ck1), (cv0, cv1)

    def chip(j):
        return lax.rem(z + j + NZ, NZ)

    def zdev(j):
        return {"seq": 2 * chip(j) + c}

    def xdev(d):
        return {"head": lax.rem(x + d, NX)}

    def ydev(d):
        return {"dp": lax.rem(y + d, NY)}

    pending = []

    def send(src, dst, send_sem, recv_sem, device, keep=True):
        copy = pltpu.make_async_remote_copy(
            src_ref=src, dst_ref=dst, send_sem=send_sem, recv_sem=recv_sem, device_id=device, device_id_type=MESH
        )
        copy.start()
        if keep:
            pending.append(copy)

    def arrived(dst, send_sem, recv_sem, device):
        pltpu.make_async_remote_copy(
            src_ref=dst, dst_ref=dst, send_sem=send_sem, recv_sem=recv_sem, device_id=device, device_id_type=MESH
        ).wait_recv()

    own = [pltpu.make_async_copy(a, b, own_sem.at[i]) for i, (a, b) in enumerate(((k_hbm, k_in), (v_hbm, v_in)))]
    loads = [
        pltpu.make_async_copy(a, b, load_sem.at[i])
        for i, (a, b) in enumerate(((q_hbm, q_ref), (u_hbm, u_ref), (o_hbm, o_ref), (hid_hbm, hid)))
    ]
    for copy in own + loads:
        copy.start()

    barrier = pltpu.get_barrier_semaphore()
    peers = [partner, zdev(1), zdev(-1)] + [xdev(d) for d in range(1, NX)] + [ydev(d) for d in range(1, NY)]
    for peer in peers:
        pl.semaphore_signal(barrier, inc=1, device_id=peer, device_id_type=MESH)
    for i, (copy, source) in enumerate(zip(own, (k_in, v_in))):
        copy.wait()
        heads = jnp.swapaxes(source[...], 0, 1).reshape(2, 4, 64, 128)
        for h in range(2):
            kbufs[h][i, pl.ds(4 * s, 4)] = heads[h]
    pl.semaphore_wait(barrier, len(peers))

    def piece_of(h, j, core, p):
        return kbufs[h].at[p // 2, pl.ds(4 * (2 * chip(j) + core) + 2 * (p % 2), 2)]

    def along(h, k, up, p):
        at = piece_of(h, -k if up else k, c, p)
        rel = (NZ - (k + 1)) if up else (k + 1)
        send(at, at, ag_send.at[h], ag_recv.at[h, rel, p], zdev(1 if up else -1), False)

    def share(h, j, p):
        at = piece_of(h, j, c, p)
        send(at, at, dd_send.at[h], dd_recv.at[h], partner, False)

    def gather_own(h, n):
        along(h, 0, True, UP[n])
        along(h, 0, False, DOWN[n])

    def gather_step(h, k, n):
        for up, p in ((True, UP[n]), (False, DOWN[n])):
            if k == 4 and n >= 2:
                continue
            j = -k if up else k
            arrived(piece_of(h, j, c, p), ag_send.at[h], ag_recv.at[h, j % NZ, p], partner)
            if k < 3 or (k == 3 and n < 2):
                along(h, k, up, p)
            share(h, j, p)

    def gather_end(h):
        arrived(pp_in.at[h], dd_send.at[h], dd_recv.at[h], partner)

    def term(h, p, owner, b):
        source = (cks, cvs)[p // 2][h]
        total = None
        for t in range(TILES):
            one = source[t, inv[2 * t + h, 4 * owner + 2 * (p % 2) + b]]
            total = one if total is None else total + one
        return total * FACTOR if p < 2 else total

    def halves(h):
        for j in (4, 3, -3, 2, -2, 1, -1, 0):
            owner = 2 * chip(j) + (1 - c)
            r = j % NZ
            for p in range(4):
                for b in range(2):
                    pp_out[h, r, p, b] = term(h, p, owner, b).astype(BF16)
            send(pp_out.at[h, r], pp_in.at[h, r], pp_send.at[h], pp_recv.at[h, r], partner, False)

    halved = set()

    def other_half(h, r):
        if (h, r) not in halved:
            halved.add((h, r))
            arrived(pp_in.at[h, r], pp_send.at[h], pp_recv.at[h, r], partner)

    def scatter_piece(h, k, up, p, received):
        j = k if up else -k
        r = j % NZ
        lane = 0 if up else 1
        owner = 2 * chip(j) + c
        other_half(h, r)
        if received:
            arrived(rs_in.at[h, lane, k, p], rs_send.at[h], rs_recv.at[h, lane, k, p], partner)
        for b in range(2):
            total = term(h, p, owner, b) + pp_in[h, r, p, b].astype(F32)
            if received:
                total = total + rs_in[h, lane, k, p, b].astype(F32)
            rs_out[h, lane, k - 1, p, b] = total.astype(BF16)
        send(
            rs_out.at[h, lane, k - 1, p], rs_in.at[h, lane, k - 1, p],
            rs_send.at[h], rs_recv.at[h, lane, k - 1, p], zdev(1 if up else -1), False,
        )

    def scatter_step(h, k, n):
        far = k == 4 or (k == 3 and n >= 2)
        scatter_piece(h, k, True, UP[n], not far)
        scatter_piece(h, k, False, DOWN[n], not far)

    def scatter_start(h):
        for k, n in ((4, 0), (4, 1), (3, 2), (3, 3)):
            scatter_step(h, k, n)

    def scatter_last(h, p):
        other_half(h, 0)
        for lane in range(2):
            arrived(rs_in.at[h, lane, 0, p], rs_send.at[h], rs_recv.at[h, lane, 0, p], partner)
        for b in range(2):
            total = term(h, p, s, b) + pp_in[h, 0, p, b].astype(F32)
            total = total + rs_in[h, 0, 0, p, b].astype(F32) + rs_in[h, 1, 0, p, b].astype(F32)
            dkv[p // 2, h, 2 * (p % 2) + b] = total.astype(BF16)

    def gate_logits(logit):
        lall[x] = logit.astype(BF16)
        for d in range(1, NX):
            send(lall.at[x], lall.at[x], lx_send.at[d - 1], lx_recv.at[d - 1], xdev(d))

    def gate_product():
        for d in range(1, NX):
            arrived(lall.at[lax.rem(x + NX - d, NX)], lx_send.at[d - 1], lx_recv.at[d - 1], partner)
        for r in range(2):
            gs[r] = nn(lall[2 * r : 2 * r + 2].reshape(32, 256), hid[...])
        send(gs.at[1 - c], pb, gp_send.at[0], gp_recv.at[0], partner)

    def gate_y():
        arrived(pb, gp_send.at[0], gp_recv.at[0], partner)
        both = gs[c] + pb[...]
        for r in range(NY):
            hb[r] = both[8 * r : 8 * r + 8]
        for d in range(1, NY):
            send(hb.at[lax.rem(y + d, NY)], yb.at[d - 1], ys_send.at[d - 1], ys_recv.at[d - 1], ydev(d))

    def gate_z():
        for d in range(1, NY):
            arrived(yb.at[d - 1], ys_send.at[d - 1], ys_recv.at[d - 1], partner)
        rows = hb[y] + yb[0] + yb[1] + yb[2]
        for r in range(NZ):
            z3[r] = rows[r : r + 1]
        for d in range(1, NZ):
            send(z3.at[chip(d)], zin.at[d - 1], zs_send.at[d - 1], zs_recv.at[d - 1], zdev(d))

    def gate_row():
        row = z3[z]
        for d in range(1, NZ):
            arrived(zin.at[d - 1], zs_send.at[d - 1], zs_recv.at[d - 1], partner)
            row = row + zin[d - 1]
        full[c, y, z] = row * SCALE
        for d in range(1, NZ):
            send(full.at[c, y, z], full.at[c, y, z], zg_send.at[d - 1], zg_recv.at[d - 1], zdev(d))

    def gate_back_y():
        for d in range(1, NZ):
            arrived(full.at[c, y, chip(-d)], zg_send.at[d - 1], zg_recv.at[d - 1], partner)
        for d in range(1, NY):
            send(full.at[c, y], full.at[c, y], yg_send.at[d - 1], yg_recv.at[d - 1], ydev(d))

    def gate_back():
        for d in range(1, NY):
            arrived(full.at[c, lax.rem(y + NY - d, NY)], yg_send.at[d - 1], yg_recv.at[d - 1], partner)
        send(full.at[c], full.at[c], gp_send.at[1], gp_recv.at[1], partner)

    def gate_end():
        arrived(full.at[1 - c], gp_send.at[1], gp_recv.at[1], partner)
        for r in range(64):
            gw[r : r + 1, :] = full[r // 32, r // 8 % 4, r % 8]

    def gather_rest(h):
        return [(gather_step, h, k, n) for k in (1, 2, 3, 4) for n in range(4) if k < 4 or n < 2]

    def scatter_rest(h):
        return [(scatter_step, h, 3, 0), (scatter_step, h, 3, 1)] + [
            (scatter_step, h, k, n) for k in (2, 1) for n in (2, 3, 0, 1)
        ]

    queue = []

    def run(count):
        for step in queue[:count]:
            step[0](*step[1:])
        del queue[:count]

    def tile(h, t, counts):
        todo = list(counts)
        attend(
            h, t, 4 * s + t, ids, valid, kbufs[h], qs, us, arow, drow, dqs, cks[h], cvs[h], lambda: run(todo.pop(0))
        )

    def invert():
        block = lax.broadcasted_iota(jnp.int32, (1, 128), 1)
        for t in range(TILES):
            for h in range(2):
                slot = jnp.full((1, 128), SLOTS, jnp.int32)
                for n in range(SLOTS):
                    at = jnp.where(valid[t, h, n] > 0, ids[t, h, n], -1)
                    slot = jnp.where(block == at, n, slot)
                inv_v[2 * t + h : 2 * t + h + 1, :] = slot
        return pltpu.make_async_copy(inv_v, inv, inv_sem)

    def drain():
        for copy in pending:
            copy.wait_send()
        del pending[:]

    for n in range(4):
        gather_own(0, n)
    for p in range(4):
        share(0, 0, p)
    gather_own(1, 0)
    for copy in loads:
        copy.wait()
    gate_logits(prepass(q_ref, u_ref, o_ref, gate_ref, tot_ref, qs, us, arow, drow, logit_ref))
    for n in range(4):
        gather_step(0, 1, n)
    gather_own(1, 1)
    gate_product()
    for n in range(4):
        gather_step(0, 2, n)
    gather_own(1, 2)
    inverse = invert()
    inverse.start()
    for h in range(2):
        for t in range(TILES):
            cks[h][t, SLOTS] = jnp.zeros((64, 128), F32)
            cvs[h][t, SLOTS] = jnp.zeros((64, 128), F32)
    gate_y()
    for n in range(4):
        gather_step(0, 3, n)
    gather_own(1, 3)
    for p in range(4):
        share(1, 0, p)
    queue += gather_rest(1)
    run(3)
    for n in range(2):
        gather_step(0, 4, n)
    gate_z()
    run(2)
    gather_end(0)
    tile(0, 0, (1, 1))
    tile(0, 1, (1, 1))
    gate_row()
    tile(0, 2, (1, 1))
    tile(0, 3, (1, 1))
    inverse.wait()
    halves(0)
    run(len(queue))
    scatter_start(0)
    gate_back_y()
    gather_end(1)
    queue += scatter_rest(0)
    tile(1, 0, (0, 1))
    tile(1, 1, (1, 1))
    gate_back()
    tile(1, 2, (2, 1))
    tile(1, 3, (2, 2))
    halves(1)
    run(len(queue))
    scatter_start(1)
    for t in range(TILES):
        pair = jnp.concatenate([dqs[h, t].reshape(64, 8, 128) for h in range(2)], axis=1)
        dq_out[pl.ds(64 * t, 64)] = pair.astype(BF16)
    stores = [pltpu.make_async_copy(dq_out, dq_hbm, store_sem.at[0])]
    stores[0].start()
    gate_end()
    stores.append(pltpu.make_async_copy(gw, gw_hbm, store_sem.at[1]))
    stores[1].start()
    for p in range(4):
        scatter_last(0, p)
    drain()
    queue += scatter_rest(1)
    run(len(queue))
    for i, (out, target) in enumerate(((dk_out, dk_hbm), (dv_out, dv_hbm))):
        for p in (2 * i, 2 * i + 1):
            scatter_last(1, p)
        out[...] = jnp.swapaxes(dkv[i].reshape(2, 256, 128), 0, 1)
        stores.append(pltpu.make_async_copy(out, target, store_sem.at[2 + i]))
        stores[-1].start()
    for h in range(2):
        for sem, count in ((ag_send, 7), (dd_send, 8), (pp_send, 8), (rs_send, 7)):
            sent = pp_out.at[h, 0:count]
            pltpu.make_async_remote_copy(
                src_ref=sent, dst_ref=sent, send_sem=sem.at[h], recv_sem=dd_recv.at[h], device_id=partner, device_id_type=MESH
            ).wait_send()
    for copy in stores:
        copy.wait()


def on_device(queries, keys, values, attn_out, out_grad, gate_values, log_totals, hidden, block_ids, block_valid):
    ids, valid = block_ids[0], block_valid[0]
    smem, vmem, hbm = (pl.BlockSpec(memory_space=m) for m in (pltpu.SMEM, pltpu.VMEM, pl.ANY))
    dma = pltpu.SemaphoreType.DMA
    piece = (2, 64, 128)
    dq, dk, dv, gw = pl.pallas_call(
        kernel,
        in_specs=[smem] * 2 + [hbm] * 5 + [vmem] * 2 + [hbm],
        out_specs=[hbm] * 4,
        out_shape=[
            jax.ShapeDtypeStruct((256, 16, 128), BF16),
            jax.ShapeDtypeStruct((256, 2, 128), BF16),
            jax.ShapeDtypeStruct((256, 2, 128), BF16),
            jax.ShapeDtypeStruct((64, 1280), F32),
        ],
        scratch_shapes=[pltpu.VMEM((256, 2, 128), BF16)] * 2
        + [pltpu.VMEM((8, 128), jnp.int32), pltpu.SMEM((8, 128), jnp.int32)]
        + [pltpu.VMEM((2, 64, 64, 128), BF16)] * 2
        + [pltpu.VMEM((256, 16, 128), BF16)] * 3
        + [pltpu.VMEM((256, 1280), BF16)]
        + [pltpu.VMEM((2, TILES, 512, 128), BF16)] * 2
        + [pltpu.VMEM((2, TILES, 8, 512), F32)] * 2
        + [pltpu.VMEM((2, TILES, 512, 128), F32), pltpu.VMEM((16, 256), F32)]
        + [pltpu.VMEM((TILES, SLOTS + 1, 64, 128), F32)] * 4
        + [pltpu.VMEM((2, NZ, 4, *piece), BF16)] * 2
        + [pltpu.VMEM((2, 2, 4, 4, *piece), BF16)] * 2
        + [pltpu.VMEM((2, 2, 4, 64, 128), BF16)] + [pltpu.VMEM((256, 2, 128), BF16)] * 2 + [pltpu.VMEM((256, 16, 128), BF16)]
        + [
            pltpu.VMEM((4, 16, 256), BF16),
            pltpu.VMEM((2, 32, 1280), F32),
            pltpu.VMEM((32, 1280), F32),
            pltpu.VMEM((4, 8, 1280), F32),
            pltpu.VMEM((3, 8, 1280), F32),
            pltpu.VMEM((8, 1, 1280), F32),
            pltpu.VMEM((7, 1, 1280), F32),
            pltpu.VMEM((2, 4, 8, 1, 1280), F32),
            pltpu.VMEM((64, 1280), F32),
        ]
        + [dma((4,)), dma((4,)), dma((2,)), dma(())]
        + [dma((2,)), dma((2, NZ, 4)), dma((2,)), dma((2,))]
        + [dma((2,)), dma((2, NZ)), dma((2,)), dma((2, 2, 4, 4))]
        + [dma((3,))] * 2
        + [dma((2,))] * 2
        + [dma((3,))] * 2
        + [dma((7,))] * 4
        + [dma((3,))] * 2,
        compiler_params=pltpu.CompilerParams(collective_id=0, has_side_effects=True, vmem_limit_bytes=62 << 20),
        name="sparse_backward",
    )(ids, valid, keys[0], values[0], queries[0], out_grad[0], attn_out[0], gate_values[0], log_totals[0], hidden[0])
    return dq[None], dk[None], dv[None], gw


def solution(mesh):
    wide = P("dp", "seq", "head", None)
    rows = P("dp", "head", "seq")
    return jax.shard_map(
        on_device,
        mesh=mesh,
        in_specs=(wide, wide, wide, wide, wide, rows, rows, P("dp", "seq", "head"), wide, wide),
        out_specs=(wide, wide, wide, P(None, "head")),
        check_vma=False,
    )
```

```python
import jax
import jax.numpy as jnp
from jax import lax
from jax.experimental import pallas as pl
from jax.experimental.pallas import tpu as pltpu
from jax.sharding import PartitionSpec as P

F32, BF16 = jnp.float32, jnp.bfloat16
MESH = pl.DeviceIdType.MESH
LOG2E = 1.4426950408889634
FACTOR = 128**-0.5
NZ, NX, NY = 8, 4, 4
TILES, SLOTS, GROUP = 4, 16, 4
SCALE = 1.0 / (4 * 4096) ** 0.5


def nt(a, b):
    return lax.dot_general(a, b, (((1,), (1,)), ((), ())), preferred_element_type=F32)


def nn(a, b):
    return jnp.dot(a, b, preferred_element_type=F32)


def tn(a, b):
    return lax.dot_general(a, b, (((0,), (0,)), ((), ())), preferred_element_type=F32)


def split3(x):
    hi = x.astype(BF16)
    rest = x - hi.astype(F32)
    mid = rest.astype(BF16)
    return hi, mid, (rest - mid.astype(F32)).astype(BF16)


def prepass(q_ref, u_ref, o_ref, gate_ref, tot_ref, qs, us, arow, drow, logit_ref):
    gate = gate_ref[...]
    shift = jnp.concatenate(split3((tot_ref[...] - jnp.log(gate)) * LOG2E), axis=0)
    token = lax.broadcasted_iota(jnp.int32, (256, 512), 0)
    lane = lax.broadcasted_iota(jnp.int32, (256, 512), 1)
    own = lax.broadcasted_iota(jnp.int32, (8, 512), 0) == lax.broadcasted_iota(jnp.int32, (8, 512), 1) % 8
    ones = jnp.ones((8, 256), BF16)
    for t in range(TILES):
        pick = jnp.where(token == 64 * t + lane // 8, 1.0, 0.0).astype(BF16)
        spread = nn(shift, pick)
        spread = spread[0:16] + spread[16:32] + spread[32:48]
        rows = pl.ds(64 * t, 64)
        up = u_ref[rows].astype(F32)
        prod = up * o_ref[rows].astype(F32)
        query = q_ref[rows].astype(F32)
        for h in range(2):
            heads = slice(8 * h, 8 * h + 8)
            qs[h, t] = query[:, heads, :].reshape(512, 128).astype(BF16)
            us[h, t] = up[:, heads, :].reshape(512, 128).astype(BF16)
            p = prod[:, heads, :].reshape(512, 128)
            high = p.astype(BF16)
            low = (p - high.astype(F32)).astype(BF16)
            delta = nt(ones, jnp.concatenate([high, low], axis=1))
            drow[h, t] = delta
            arow[h, t] = jnp.broadcast_to(jnp.sum(jnp.where(own, spread[heads], 0.0), axis=0, keepdims=True), (8, 512))
            mine = jnp.where(own, delta, 0.0)
            high = mine.astype(BF16)
            low = (mine - high.astype(F32)).astype(BF16)
            back = nt(jnp.concatenate([high, low], axis=0), pick)
            back = back[0:8] + back[8:16]
            if t == 0:
                logit_ref[heads, :] = back
            else:
                logit_ref[heads, :] += back
    return logit_ref[...] * gate * (1.0 - gate)


def attend(h, t, tile_number, ids, valid, kbuf, qs, us, arow, drow, dqs, terms, between):
    query, up = qs[h, t], us[h, t]
    shift, delta = arow[h, t][0:1], drow[h, t][0:1]
    ahead = lax.broadcasted_iota(jnp.int32, (64, 512), 1) // 8 - lax.broadcasted_iota(jnp.int32, (64, 512), 0)
    dq = None
    for first in range(0, SLOTS, GROUP):
        picked = [ids[t, h, first + k] for k in range(GROUP)]
        key = jnp.concatenate([kbuf[0, m] for m in picked], axis=0)
        value = jnp.concatenate([kbuf[1, m] for m in picked], axis=0)
        score = nt(key, query)
        grad = nt(value, up)
        probs, dscores = [], []
        for k in range(GROUP):
            least = jnp.where(valid[t, h, first + k] > 0, (picked[k] - tile_number) * 64, 1 << 20)
            part = slice(64 * k, 64 * k + 64)
            prob = jnp.exp2(jnp.where(ahead >= least, score[part] * (FACTOR * LOG2E) - shift, -jnp.inf))
            probs.append(prob.astype(BF16))
            dscores.append((prob * (grad[part] - delta)).astype(BF16))
        prob = jnp.concatenate(probs, axis=0)
        dscore = jnp.concatenate(dscores, axis=0)
        dv = nn(prob, up)
        dk = nn(dscore, query)
        for k in range(GROUP):
            terms[1, t, first + k] = dv[64 * k : 64 * k + 64]
            terms[0, t, first + k] = dk[64 * k : 64 * k + 64] * FACTOR
        more = tn(key, dscore)
        dq = more if dq is None else dq + more
        if first // GROUP % 2 == 1:
            between()
    dqs[h, t] = (dq * FACTOR).T


def kernel(
    ids_hbm, valid_hbm, k_hbm, v_hbm, q_hbm, u_hbm, o_hbm, gate_hbm, tot_hbm, hid_hbm,
    dq_hbm, dk_hbm, dv_hbm, gw_hbm,
    dq_out, dk_out, dv_out, gw, ids, valid, gate_ref, tot_ref, k_in, v_in, inv_v, inv, k0, k1, q_ref, u_ref, o_ref, hid, qs, us, arow, drow, dqs, logit_ref,
    terms0, terms1, pp_out, pp_in, po_out, po_in, rs_out, rs_in, rs_fin, dkv,
    lall, gs, pb, hb, yb, z3, zin, full,
    store_sem, small_sem, load_sem, own_sem, inv_sem, ag_send, ag_recv, dd_send, dd_recv, os_recv, pp_send, pp_recv, rs_send, rs_recv, fin_recv,
    lx_send, lx_recv, gp_send, gp_recv, ys_send, ys_recv, zs_send, zs_recv, zg_send, zg_recv, yg_send, yg_recv,
):
    s = lax.axis_index("seq")
    x = lax.axis_index("head")
    y = lax.axis_index("dp")
    z = s // 2
    c = s % 2
    partner = {"seq": 2 * z + (1 - c)}
    d = 1 - 2 * c
    kbufs, terms = (k0, k1), (terms0, terms1)

    def chip(j):
        return lax.rem(z + j + NZ, NZ)

    def zdev(j):
        return {"seq": 2 * chip(j) + c}

    def xdev(d):
        return {"head": lax.rem(x + d, NX)}

    def ydev(d):
        return {"dp": lax.rem(y + d, NY)}

    pending = []

    def send(src, dst, send_sem, recv_sem, device, keep=True):
        copy = pltpu.make_async_remote_copy(
            src_ref=src, dst_ref=dst, send_sem=send_sem, recv_sem=recv_sem, device_id=device, device_id_type=MESH
        )
        copy.start()
        if keep:
            pending.append(copy)

    def arrived(dst, send_sem, recv_sem, device):
        pltpu.make_async_remote_copy(
            src_ref=dst, dst_ref=dst, send_sem=send_sem, recv_sem=recv_sem, device_id=device, device_id_type=MESH
        ).wait_recv()

    own = [pltpu.make_async_copy(a, b, own_sem.at[i]) for i, (a, b) in enumerate(((k_hbm, k_in), (v_hbm, v_in)))]
    loads = [
        pltpu.make_async_copy(a, b, load_sem.at[i])
        for i, (a, b) in enumerate(((q_hbm, q_ref), (u_hbm, u_ref), (o_hbm, o_ref), (hid_hbm, hid)))
    ]
    small = [
        pltpu.make_async_copy(a, b, small_sem.at[i])
        for i, (a, b) in enumerate(((gate_hbm, gate_ref), (tot_hbm, tot_ref), (ids_hbm, ids), (valid_hbm, valid)))
    ]
    for copy in own + loads + small:
        copy.start()

    barrier = pltpu.get_barrier_semaphore()
    peers = [partner] + [{"seq": 2 * chip(j) + core} for j in (1, -1) for core in range(2)] + [xdev(d) for d in range(1, NX)] + [ydev(d) for d in range(1, NY)]
    for peer in peers:
        pl.semaphore_signal(barrier, inc=1, device_id=peer, device_id_type=MESH)
    for i, (copy, source) in enumerate(zip(own, (k_in, v_in))):
        copy.wait()
        heads = jnp.swapaxes(source[...], 0, 1).reshape(2, 4, 64, 128)
        for h in range(2):
            kbufs[h][i, pl.ds(4 * s, 4)] = heads[h]
    for h in range(2):
        for i in range(2):
            for t in range(TILES):
                terms[h][i, t, SLOTS] = jnp.zeros((64, 128), F32)
    pl.semaphore_wait(barrier, len(peers))

    ahead = zdev(d)

    def kind(n):
        return lax.rem(n // 2 + c, 2)

    def spot(h, k, q, n):
        return kbufs[h].at[kind(n), pl.ds(4 * (2 * chip(-k * d) + (1 - c if q else c)) + 2 * (n % 2), 2)]

    def along(h, k, q, n):
        at = spot(h, k, q, n)
        send(at, at, ag_send.at[h], ag_recv.at[h, k, q, n], ahead, False)

    def share_own(h):
        for n in (2, 3, 0, 1):
            at = spot(h, 0, 0, n)
            send(at, at, dd_send.at[h], os_recv.at[h, n], partner, False)

    def gather_own(h, q):
        for n in range(4):
            if q:
                arrived(spot(h, 0, 1, n), dd_send.at[h], os_recv.at[h, (n + 2) % 4], partner)
            along(h, 0, q, n)

    def gather_step(h, k, q, first):
        for n in (first, first + 1):
            at = spot(h, k, q, n)
            arrived(at, ag_send.at[h], ag_recv.at[h, k - 1, q, n], partner)
            if k < 3 or (k == 3 and n < 2):
                along(h, k, q, n)
        for n in (first, first + 1):
            at = spot(h, k, q, n)
            send(at, at, dd_send.at[h], dd_recv.at[h], partner, False)

    def gather_end(h):
        arrived(kbufs[h].at[0, pl.ds(0, 56)], dd_send.at[h], dd_recv.at[h], partner)

    def term(h, i, half, owner, b):
        total = None
        for t in range(TILES):
            one = terms[h][i, t, inv[2 * t + h, 4 * owner + 2 * half + b]]
            total = one if total is None else total + one
        return total

    def halves(h):
        for k in (4, 3, 2, 1):
            count = 4 if k < 4 else 2
            for n in range(count):
                for plane in range(2):
                    for b in range(2):
                        one = term(h, lax.rem(n // 2 + 1 - c, 2), n % 2, 2 * chip(-k * d) + plane, b)
                        pp_out[h, k - 1, n, plane, b] = one.astype(BF16)
            out, into = (a.at[h, k - 1, pl.ds(0, count)] for a in (pp_out, pp_in))
            send(out, into, pp_send.at[h], pp_recv.at[h, k], partner, False)
        for p in range(4):
            for b in range(2):
                po_out[h, p, b] = term(h, p // 2, p % 2, 2 * z + (1 - c), b).astype(BF16)
        send(po_out.at[h], po_in.at[h], pp_send.at[h], pp_recv.at[h, 0], partner, False)

    halved = set()

    def other_half(h, k):
        if (h, k) not in halved:
            halved.add((h, k))
            into = pp_in.at[h, k - 1, pl.ds(0, 4 if k < 4 else 2)] if k else po_in.at[h]
            arrived(into, pp_send.at[h], pp_recv.at[h, k], partner)

    def scatter_step(h, k, n):
        received = not (k == 4 or (k == 3 and n >= 2))
        other_half(h, k)
        for plane in range(2):
            if received:
                arrived(rs_in.at[h, k - 1, n, plane], rs_send.at[h], rs_recv.at[h, k - 1, n, plane], partner)
            for b in range(2):
                total = term(h, kind(n), n % 2, 2 * chip(k * d) + plane, b) + pp_in[h, k - 1, n, plane, b].astype(F32)
                if received:
                    total = total + rs_in[h, k - 1, n, plane, b].astype(F32)
                rs_out[h, k - 1, n, plane, b] = total.astype(BF16)
            if k > 1:
                into, sem, device = rs_in.at[h, k - 2, n, plane], rs_recv.at[h, k - 2, n, plane], ahead
            else:
                p = lax.rem(n + 2 * c, 4)
                into, sem, device = rs_fin.at[h, c, p], fin_recv.at[h, c, p], {"seq": 2 * chip(d) + plane}
            send(rs_out.at[h, k - 1, n, plane], into, rs_send.at[h], sem, device, False)

    def scatter_start(h):
        for k, n in ((4, 0), (4, 1), (3, 2), (3, 3)):
            scatter_step(h, k, n)

    def scatter_last(h, p):
        other_half(h, 0)
        for core in range(2):
            arrived(rs_fin.at[h, core, p], rs_send.at[h], fin_recv.at[h, core, p], partner)
        for b in range(2):
            total = term(h, p // 2, p % 2, s, b) + po_in[h, p, b].astype(F32)
            total = total + rs_fin[h, 0, p, b].astype(F32) + rs_fin[h, 1, p, b].astype(F32)
            dkv[p // 2, h, 2 * (p % 2) + b] = total.astype(BF16)

    def gate_logits(logit):
        lall[x] = logit.astype(BF16)
        for d in range(1, NX):
            send(lall.at[x], lall.at[x], lx_send.at[d - 1], lx_recv.at[d - 1], xdev(d))

    def gate_product():
        for d in range(1, NX):
            arrived(lall.at[lax.rem(x + NX - d, NX)], lx_send.at[d - 1], lx_recv.at[d - 1], partner)
        for r in range(2):
            gs[r] = nn(lall[2 * r : 2 * r + 2].reshape(32, 256), hid[...])
        send(gs.at[1 - c], pb, gp_send.at[0], gp_recv.at[0], partner)

    def gate_y():
        arrived(pb, gp_send.at[0], gp_recv.at[0], partner)
        both = gs[c] + pb[...]
        for r in range(NY):
            hb[r] = both[8 * r : 8 * r + 8]
        for d in range(1, NY):
            send(hb.at[lax.rem(y + d, NY)], yb.at[d - 1], ys_send.at[d - 1], ys_recv.at[d - 1], ydev(d))

    def gate_z():
        for d in range(1, NY):
            arrived(yb.at[d - 1], ys_send.at[d - 1], ys_recv.at[d - 1], partner)
        rows = hb[y] + yb[0] + yb[1] + yb[2]
        for r in range(NZ):
            z3[r] = rows[r : r + 1]
        for d in range(1, NZ):
            send(z3.at[chip(d)], zin.at[d - 1], zs_send.at[d - 1], zs_recv.at[d - 1], zdev(d))

    def gate_row():
        row = z3[z]
        for d in range(1, NZ):
            arrived(zin.at[d - 1], zs_send.at[d - 1], zs_recv.at[d - 1], partner)
            row = row + zin[d - 1]
        full[c, y, z] = row * SCALE
        for d in range(1, NZ):
            send(full.at[c, y, z], full.at[c, y, z], zg_send.at[d - 1], zg_recv.at[d - 1], zdev(d))

    def gate_back_y():
        for d in range(1, NZ):
            arrived(full.at[c, y, chip(-d)], zg_send.at[d - 1], zg_recv.at[d - 1], partner)
        for d in range(1, NY):
            send(full.at[c, y], full.at[c, y], yg_send.at[d - 1], yg_recv.at[d - 1], ydev(d))

    def gate_back():
        for d in range(1, NY):
            arrived(full.at[c, lax.rem(y + NY - d, NY)], yg_send.at[d - 1], yg_recv.at[d - 1], partner)
        send(full.at[c], full.at[c], gp_send.at[1], gp_recv.at[1], partner)

    def gate_end():
        arrived(full.at[1 - c], gp_send.at[1], gp_recv.at[1], partner)
        for r in range(64):
            gw[r : r + 1, :] = full[r // 32, r // 8 % 4, r % 8]

    def gather_rest(h):
        return [(gather_step, h, k, q, n) for k in (1, 2, 3, 4) for q in (0, 1) for n in (0, 2) if k < 4 or n < 2]

    def scatter_rest(h):
        return [(scatter_step, h, 3, 0), (scatter_step, h, 3, 1)] + [
            (scatter_step, h, k, n) for k in (2, 1) for n in (2, 3, 0, 1)
        ]

    queue = []

    def run(count):
        for step in queue[:count]:
            step[0](*step[1:])
        del queue[:count]

    def tile(h, t, counts):
        todo = list(counts)
        attend(
            h, t, 4 * s + t, ids, valid, kbufs[h], qs, us, arow, drow, dqs, terms[h], lambda: run(todo.pop(0))
        )

    def invert():
        block = lax.broadcasted_iota(jnp.int32, (1, 128), 1)
        for t in range(TILES):
            for h in range(2):
                slot = jnp.full((1, 128), SLOTS, jnp.int32)
                for n in range(SLOTS):
                    at = jnp.where(valid[t, h, n] > 0, ids[t, h, n], -1)
                    slot = jnp.where(block == at, n, slot)
                inv_v[2 * t + h : 2 * t + h + 1, :] = slot
        return pltpu.make_async_copy(inv_v, inv, inv_sem)

    def drain():
        for copy in pending:
            copy.wait_send()
        del pending[:]

    gather_own(0, 0)
    share_own(0)
    share_own(1)
    gather_own(0, 1)
    for copy in loads + small:
        copy.wait()
    gate_logits(prepass(q_ref, u_ref, o_ref, gate_ref, tot_ref, qs, us, arow, drow, logit_ref))
    queue += gather_rest(0)
    run(4)
    gate_product()
    run(4)
    inverse = invert()
    inverse.start()
    gate_y()
    run(4)
    gather_own(1, 0)
    gather_own(1, 1)
    run(2)
    gate_z()
    queue += gather_rest(1)
    run(1)
    gather_end(0)
    tile(0, 0, (1, 1))
    tile(0, 1, (2, 1))
    gate_row()
    tile(0, 2, (1, 1))
    tile(0, 3, (1, 1))
    inverse.wait()
    halves(0)
    run(2)
    scatter_start(0)
    run(len(queue))
    gate_back_y()
    gather_end(1)
    queue += scatter_rest(0)
    tile(1, 0, (1, 1))
    tile(1, 1, (1, 1))
    gate_back()
    tile(1, 2, (1, 1))
    tile(1, 3, (1, 1))
    halves(1)
    run(len(queue))
    scatter_start(1)
    for t in range(TILES):
        pair = jnp.concatenate([dqs[h, t].reshape(64, 8, 128) for h in range(2)], axis=1)
        dq_out[pl.ds(64 * t, 64)] = pair.astype(BF16)
    stores = [pltpu.make_async_copy(dq_out, dq_hbm, store_sem.at[0])]
    stores[0].start()
    gate_end()
    stores.append(pltpu.make_async_copy(gw, gw_hbm, store_sem.at[1]))
    stores[1].start()
    queue += scatter_rest(1)
    run(4)
    drain()
    for p in range(4):
        scatter_last(0, p)
    run(len(queue))
    for i, (out, target) in enumerate(((dk_out, dk_hbm), (dv_out, dv_hbm))):
        for p in (2 * i, 2 * i + 1):
            scatter_last(1, p)
        out[...] = jnp.swapaxes(dkv[i].reshape(2, 256, 128), 0, 1)
        stores.append(pltpu.make_async_copy(out, target, store_sem.at[2 + i]))
        stores[-1].start()
    for h in range(2):
        for sem, count in ((ag_send, 56), (dd_send, 64), (pp_send, 64), (rs_send, 56)):
            sent = kbufs[h].at[0, pl.ds(0, count)]
            pltpu.make_async_remote_copy(
                src_ref=sent, dst_ref=sent, send_sem=sem.at[h], recv_sem=dd_recv.at[h], device_id=partner, device_id_type=MESH
            ).wait_send()
    for copy in stores:
        copy.wait()


def hand_over(dq, dk, dv, gw, dq_out, dk_out, dv_out, gw_out, dq_v, dk_v, dv_v, gw_v, in_sem, out_sem):
    arrays = ((dk, dk_v, dk_out), (dv, dv_v, dv_out), (gw, gw_v, gw_out), (dq, dq_v, dq_out))
    inward = [pltpu.make_async_copy(a, v, in_sem.at[i]) for i, (a, v, _) in enumerate(arrays)]
    outward = [pltpu.make_async_copy(v, b, out_sem.at[i]) for i, (_, v, b) in enumerate(arrays)]
    for copy in inward:
        copy.start()
    for arrive, leave in zip(inward, outward):
        arrive.wait()
        leave.start()
    for copy in outward:
        copy.wait()


def on_device(queries, keys, values, attn_out, out_grad, gate_values, log_totals, hidden, block_ids, block_valid):
    ids, valid = block_ids[0], block_valid[0]
    hbm = pl.BlockSpec(memory_space=pltpu.HBM)
    results = [
        jax.ShapeDtypeStruct((256, 16, 128), BF16),
        jax.ShapeDtypeStruct((256, 2, 128), BF16),
        jax.ShapeDtypeStruct((256, 2, 128), BF16),
        jax.ShapeDtypeStruct((64, 1280), F32),
    ]
    dma = pltpu.SemaphoreType.DMA
    piece = (2, 64, 128)
    sums = pl.pallas_call(
        kernel,
        in_specs=[hbm] * 10,
        out_specs=[hbm] * 4,
        out_shape=results,
        scratch_shapes=[pltpu.VMEM(a.shape, a.dtype) for a in results]
        + [pltpu.SMEM((4, 2, 16), jnp.int32)] * 2
        + [pltpu.VMEM((16, 256), F32)] * 2
        + [pltpu.VMEM((256, 2, 128), BF16)] * 2
        + [pltpu.VMEM((8, 128), jnp.int32), pltpu.SMEM((8, 128), jnp.int32)]
        + [pltpu.VMEM((2, 64, 64, 128), BF16)] * 2
        + [pltpu.VMEM((256, 16, 128), BF16)] * 3
        + [pltpu.VMEM((256, 1280), BF16)]
        + [pltpu.VMEM((2, TILES, 512, 128), BF16)] * 2
        + [pltpu.VMEM((2, TILES, 8, 512), F32)] * 2
        + [pltpu.VMEM((2, TILES, 512, 128), F32), pltpu.VMEM((16, 256), F32)]
        + [pltpu.VMEM((2, TILES, SLOTS + 1, 64, 128), F32)] * 2
        + [pltpu.VMEM((2, 4, 4, 2, *piece), BF16)] * 2
        + [pltpu.VMEM((2, 4, *piece), BF16)] * 2
        + [pltpu.VMEM((2, 4, 4, 2, *piece), BF16), pltpu.VMEM((2, 3, 4, 2, *piece), BF16)]
        + [pltpu.VMEM((2, 2, 4, *piece), BF16)]
        + [pltpu.VMEM((2, 2, 4, 64, 128), BF16)]
        + [
            pltpu.VMEM((4, 16, 256), BF16),
            pltpu.VMEM((2, 32, 1280), F32),
            pltpu.VMEM((32, 1280), F32),
            pltpu.VMEM((4, 8, 1280), F32),
            pltpu.VMEM((3, 8, 1280), F32),
            pltpu.VMEM((8, 1, 1280), F32),
            pltpu.VMEM((7, 1, 1280), F32),
            pltpu.VMEM((2, 4, 8, 1, 1280), F32),
        ]
        + [dma((4,)), dma((4,)), dma((4,)), dma((2,)), dma(())]
        + [dma((2,)), dma((2, 4, 2, 4)), dma((2,)), dma((2,)), dma((2, 4))]
        + [dma((2,)), dma((2, 5)), dma((2,)), dma((2, 3, 4, 2)), dma((2, 2, 4))]
        + [dma((3,))] * 2
        + [dma((2,))] * 2
        + [dma((3,))] * 2
        + [dma((7,))] * 4
        + [dma((3,))] * 2,
        compiler_params=pltpu.CompilerParams(collective_id=0, has_side_effects=True, vmem_limit_bytes=62 << 20),
        name="sparse_backward",
    )(ids, valid, keys[0], values[0], queries[0], out_grad[0], attn_out[0], gate_values[0], log_totals[0], hidden[0])
    dq, dk, dv, gw = pl.pallas_call(
        hand_over,
        in_specs=[hbm] * 4,
        out_specs=[hbm] * 4,
        out_shape=results,
        scratch_shapes=[pltpu.VMEM(a.shape, a.dtype) for a in results] + [dma((4,)), dma((4,))],
        compiler_params=pltpu.CompilerParams(vmem_limit_bytes=62 << 20),
        name="hand_over",
    )(*sums)
    return dq[None], dk[None], dv[None], gw


def solution(mesh):
    wide = P("dp", "seq", "head", None)
    rows = P("dp", "head", "seq")
    return jax.shard_map(
        on_device,
        mesh=mesh,
        in_specs=(wide, wide, wide, wide, wide, rows, rows, P("dp", "seq", "head"), wide, wide),
        out_specs=(wide, wide, wide, P(None, "head")),
        check_vma=False,
    )
```
